32 devices in a mesh: grid: 8 (over y, x, core), rows: 4 (over z).
Axes of the slice: x: 2, y: 2, z: 4, core: 2. Of those that a mesh axis runs over, the one named last changes fastest.
Arguments:
- density: bfloat16 [32, 128, 4096], P(None, 'rows', 'grid'), as said below
- basis_values: bfloat16 [16, 16, 128, 512], P('grid', None, 'rows'), may hold values from -0.59765625 to 0.59765625
- grid_points: float32 [16, 3, 512], P('grid'), may hold values from -4 to 4
- grid_weights: float32 [16, 512], P('grid'), may hold values from 0.05 to 1
- screened_blocks: int32 [16, 16], P('grid'), may hold values from 0 to 31, as said below
Outputs:
- exchange: float32 [32, 128, 4096], P(None, 'rows', 'grid')
The draws below stay inside these ranges and needn't reach their ends.
Inputs may be any that keep to these rules, and one draw needn't show every extreme that they name: density is symmetric: density[a, i, b * 128 + j] equals density[b, j, a * 128 + i]. `screened_blocks`: each row holds 16 distinct block numbers.
All inputs are finite; a program needn't handle non-finite values.
Results may differ from the reference program's by a relative error of at most 0.00055.
The reference program's roundings to bfloat16 on the way count: a program that leaves them out, or rounds other values in their place, can miss the bound.
Values may be sent and summed in bfloat16 or wider, within the bound.
A program may use at most 128 MiB of HBM per device.

```python
import math
import jax
import jax.numpy as jnp
from jax import lax

NBF = 4096
BS = 128
SIG = 16
PTS = 512
NBLK = 32
NBATCH = 16


def draw_density(key, part):
    key_off, key_diag = jax.random.split(jax.random.fold_in(key, 11), 2)
    noise = jax.random.normal(key_off, (NBF, NBF), jnp.float32) * (0.6 * (2.0 * NBF) ** (-0.5))
    dens = noise + noise.T
    diagonal = jax.random.uniform(key_diag, (NBF,), jnp.float32, 1.6, 2.6)
    dens = dens + jnp.diag(diagonal)
    return dens.reshape(NBF // BS, BS, NBF).astype(jnp.bfloat16)


def draw_screened_blocks(key, part):
    keys = jax.random.split(jax.random.fold_in(key, 7), NBATCH)
    picks = jax.vmap(lambda one_key: jax.random.permutation(one_key, NBF // BS)[:SIG])(keys)
    return picks.astype(jnp.int32)


def level_of(own_key, shape, cuts, least, largest):
    level = 1.0
    for position, shards_of in cuts:
        draws = jax.random.uniform(jax.random.fold_in(jax.random.fold_in(own_key, 6), position), (shards_of,), jnp.float32, least / len(cuts), largest / len(cuts))
        level = level * jnp.repeat(jnp.exp(draws), shape[position] // shards_of).reshape((-1,) + (1,) * (len(shape) - 1 - position))
    return level


def scatter_about(stream_key, extent, deviation, limit, cuts=(), dtype=jnp.bfloat16):
    values = deviation * jax.random.normal(stream_key, extent, jnp.float32)
    if cuts:
        values = values * level_of(stream_key, extent, cuts, -0.22, 0.18)
    return jnp.clip(values, -limit, limit).astype(dtype)


def setup_inputs(seed: int = 0) -> dict:
    key_of = jax.random.split(jax.random.key(seed), 6)
    return {
        "density": draw_density(jax.random.fold_in(key_of[5], 71), 0),
        "basis_values": scatter_about(key_of[1], (NBATCH, SIG, BS, PTS), 0.1, 0.59765625, ((0, 8), (2, 4))),
        "grid_points": jnp.clip(jax.random.uniform(key_of[2], (NBATCH, 3, PTS), jnp.float32, -4.0, 4.0) * level_of(key_of[2], (NBATCH, 3, PTS), ((0, 8),), -0.4, 0.0), -4.0, 4.0),
        "grid_weights": jnp.clip(jnp.exp(math.log(1.0) - 2.9957323 * jax.random.uniform(key_of[3], (NBATCH, PTS), jnp.float32) ** level_of(key_of[3], (NBATCH, PTS), ((0, 8),), -0.2, 0.2)), 0.05, 1.0),
        "screened_blocks": draw_screened_blocks(jax.random.fold_in(key_of[5], 71), 0),
    }


def reference(density, basis_values, grid_points, grid_weights, screened_blocks):
    dense = density.reshape(NBLK, BS, NBLK, BS)

    def one_batch(totals, items):
        values, places, weights, blocks = items
        chosen = dense[blocks][:, :, blocks, :].reshape(SIG * BS, SIG * BS)
        flat = values.reshape(SIG * BS, PTS)
        fmat = jnp.dot(chosen, flat, preferred_element_type=jnp.float32).astype(jnp.bfloat16)
        intersection = jnp.dot(flat.T, fmat, preferred_element_type=jnp.float32)
        diffs = places[:, :, None] - places[:, None, :]
        kern = 1.0 / jnp.sqrt(lax.optimization_barrier(jnp.sum(diffs * diffs, axis=0)) + 0.5)
        mixed = (weights[:, None] * kern * intersection).astype(jnp.bfloat16)
        potential = (jnp.dot(flat, mixed, preferred_element_type=jnp.float32) * weights[None, :]).astype(jnp.bfloat16)
        block_k = jnp.dot(flat, potential.T, preferred_element_type=jnp.float32).reshape(SIG, BS, SIG, BS)
        totals = totals.at[blocks[:, None], :, blocks[None, :], :].add(block_k.transpose(0, 2, 1, 3))
        return (totals, None)
    start_totals = jnp.zeros((NBLK, BS, NBLK, BS), jnp.float32)
    totals, unused = lax.scan(one_batch, start_totals, (basis_values, grid_points, grid_weights, screened_blocks))
    return totals.reshape(NBLK, BS, NBLK * BS)
```

```python
import functools

import jax
import jax.numpy as jnp
from jax import lax
from jax.experimental import pallas as pl
from jax.experimental.pallas import tpu as pltpu
from jax.sharding import PartitionSpec as P

MESH = pl.DeviceIdType.MESH
F32 = jnp.float32
BF16 = jnp.bfloat16
CORES = 2
GROUP = 128
LEVELS = 32767.0
TINY = 2.0 ** -110


def kernel(
    ngrid, nrows, sel_ref, part_ref, cut_ref, inv_ref, p_ref, x_ref, pts_ref, ptst_ref, w_ref, wt_ref, out_ref,
    p_all, x_all, psel, fm_send, fm_all, mixed, xpad, pot, lhs, rhs, pair_send, pair_recv,
    q_send, q_recv, s_send, s_recv,
    p_out, p_pair, p_in, x_up, x_down, x_in, local, fm_out, fm_in, m_up, m_down, m_in,
    pair_out, pair_in, q_out, q_in, s_out, s_in,
):
    me = lax.axis_index("grid")
    z = lax.axis_index("rows")
    core = lax.rem(me, CORES)
    chip = me // CORES
    nchip = ngrid // CORES
    partner = chip * CORES + (CORES - 1 - core)
    nblk, bpd, rows, bs = p_ref.shape
    nb, nsig, _, npts = x_ref.shape
    cols = bpd * bs
    split = nrows // nb
    half = npts // split

    def peer(k):
        return lax.rem(chip + k, nchip) * CORES + core

    def origin(k):
        return lax.rem(chip + nchip - k, nchip) * CORES + core

    barrier = pltpu.get_barrier_semaphore()
    for k in range(1, nrows):
        pl.semaphore_signal(barrier, inc=1, device_id=(me, lax.rem(z + k, nrows)), device_id_type=MESH)
    for k in range(1, nchip):
        pl.semaphore_signal(barrier, inc=1, device_id=(peer(k), z), device_id_type=MESH)
    pl.semaphore_signal(barrier, inc=1, device_id=(partner, z), device_id_type=MESH)
    pl.semaphore_wait(barrier, nrows - 1 + nchip - 1 + 1)

    def remote(src, dst, send, recv, device):
        return pltpu.make_async_remote_copy(
            src_ref=src, dst_ref=dst, send_sem=send, recv_sem=recv, device_id=device, device_id_type=MESH
        )

    def x_slot(batch, owner):
        return x_all.at[batch, :, pl.ds(pl.multiple_of(owner * rows, rows), rows), :]

    def x_copy(batch, owner, step, src=None):
        up = step > 0
        sems = x_up if up else x_down
        return remote(
            x_slot(batch, owner) if src is None else src, x_slot(batch, owner),
            sems.at[batch, owner], x_in.at[batch, owner], (me, z + step),
        )

    for batch in range(nb):
        mine = x_ref.at[batch]

        @pl.when(z > 0)
        def _():
            x_copy(batch, z, -1, mine).start()

        @pl.when(z < nrows - 1)
        def _():
            x_copy(batch, z, 1, mine).start()

    def p_copy(k):
        return remote(p_ref, p_all.at[me], p_out.at[k], p_in.at[me], (peer(k), z))

    def p_wait(k):
        return remote(p_ref, p_all.at[origin(k)], p_out.at[k], p_in.at[origin(k)], (peer(k), z))

    def p_forward(k):
        src = p_ref if k == 0 else p_all.at[origin(k)]
        return remote(src, p_all.at[origin(k)], p_pair.at[k], p_in.at[origin(k)], (partner, z))

    def p_pair_wait(k):
        slot = lax.rem(chip + nchip - k, nchip) * CORES + (CORES - 1 - core)
        return remote(p_ref, p_all.at[slot], p_pair.at[k], p_in.at[slot], (partner, z))

    for k in range(1, nchip):
        p_copy(k).start()
    p_forward(0).start()

    locals_ = [pltpu.make_async_copy(p_ref, p_all.at[me], local.at[0])]
    for batch in range(nb):
        locals_.append(pltpu.make_async_copy(x_ref.at[batch], x_slot(batch, z), local.at[1 + batch]))
        locals_.append(
            pltpu.make_async_copy(x_ref.at[batch], xpad.at[batch, pl.ds(0, nsig)], local.at[1 + nb + batch])
        )
    for copy in locals_:
        copy.start()
    for batch in range(nb):
        xpad[batch, nsig] = jnp.zeros((rows, npts), BF16)
        pot[batch, nsig] = jnp.zeros((bs, npts), BF16)
    for copy in locals_:
        copy.wait()

    for batch in range(nb):
        def fill(block, carry):
            lhs[pl.ds(pl.multiple_of(block * rows, rows), rows), batch * npts:(batch + 1) * npts] = xpad[
                batch, inv_ref[batch, block]
            ]
            return carry
        lax.fori_loop(0, nblk, fill, 0)

    def x_arrive(dist, batch):
        @pl.when(z + dist < nrows)
        def _():
            x_copy(batch, z + dist, -1).wait_recv()

            @pl.when(z > 0)
            def _():
                x_copy(batch, z + dist, -1).start()

        @pl.when(z - dist >= 0)
        def _():
            x_copy(batch, z - dist, 1).wait_recv()

            @pl.when(z < nrows - 1)
            def _():
                x_copy(batch, z - dist, 1).start()

    for dist in range(1, nrows - 1):
        for batch in range(nb):
            x_arrive(dist, batch)
    for k in range(1, nchip):
        p_wait(k).wait_recv()
        p_forward(k).start()
    for k in range(nchip):
        p_pair_wait(k).wait_recv()

    def fm_slot(owner):
        return fm_all.at[:, pl.ds(pl.multiple_of(owner * rows, rows), rows), :]

    def fm_copy(owner):
        return remote(fm_send.at[owner], fm_slot(z), fm_out.at[owner], fm_in.at[z], (me, owner))

    def fm_wait(source):
        return remote(fm_send.at[0], fm_slot(source), fm_out.at[0], fm_in.at[source], (me, source))

    for batch in range(nb):
        x_arrive(nrows - 1, batch)

        def pick(s, carry):
            row = sel_ref[batch, s]
            for t in range(nsig):
                psel[pl.ds(pl.multiple_of(s * rows, rows), rows), t * bs:(t + 1) * bs] = p_all[
                    part_ref[batch, t], row, cut_ref[batch, t]
                ]
            return carry
        lax.fori_loop(0, nsig, pick, 0)
        for h in range(split):
            got = jnp.dot(
                psel[...], x_all[batch, :, :, h * half:(h + 1) * half].reshape(nsig * bs, half),
                preferred_element_type=F32,
            )
            fm_send[batch * split + h] = got.astype(BF16).reshape(nsig, rows, half)
        for h in range(split):
            owner = batch * split + h

            @pl.when(z != owner)
            def _():
                fm_copy(owner).start()

            @pl.when(z == owner)
            def _():
                own = pltpu.make_async_copy(fm_send.at[owner], fm_slot(z), local.at[0])
                own.start()
                own.wait()

    for source in range(nrows):
        @pl.when(z != source)
        def _():
            fm_wait(source).wait_recv()

    bmine = z // split
    hmine = lax.rem(z, split)
    lanes = pl.ds(pl.multiple_of(hmine * half, half), half)
    tile = npts // 4
    for piece in range(4):
        q = slice(piece * tile, (piece + 1) * tile)
        inter = lax.dot_general(
            x_all[bmine, :, :, q].reshape(nsig * bs, tile), fm_all[...].reshape(nsig * bs, half),
            (((0,), (0,)), ((), ())), preferred_element_type=F32,
        )
        dist2 = None
        for axis in range(3):
            diff = ptst_ref[bmine, q, axis:axis + 1] - pts_ref[bmine, axis:axis + 1, lanes]
            dist2 = diff * diff if dist2 is None else dist2 + diff * diff
        kern = 1.0 / jnp.sqrt(dist2 + 0.5)
        mixed[z, q, :] = (wt_ref[bmine, q, :] * kern * inter).astype(BF16)

    def m_copy(owner, step):
        sems = m_up if step > 0 else m_down
        return remote(mixed.at[owner], mixed.at[owner], sems.at[owner], m_in.at[owner], (me, z + step))

    @pl.when(z > 0)
    def _():
        m_copy(z, -1).start()

    @pl.when(z < nrows - 1)
    def _():
        m_copy(z, 1).start()

    for dist in range(1, nrows):
        @pl.when(z + dist < nrows)
        def _():
            m_copy(z + dist, -1).wait_recv()

            @pl.when(z > 0)
            def _():
                m_copy(z + dist, -1).start()

        @pl.when(z - dist >= 0)
        def _():
            m_copy(z - dist, 1).wait_recv()

            @pl.when(z < nrows - 1)
            def _():
                m_copy(z - dist, 1).start()

    for batch in range(nb):
        for h in range(split):
            cut = slice(h * half, (h + 1) * half)

            def fill_pot(part, carry):
                some = pl.ds(part * 4, 4)
                got = jnp.dot(
                    x_all[batch, some].reshape(4 * bs, npts), mixed[batch * split + h], preferred_element_type=F32
                ) * w_ref[batch, :, cut]
                pot[batch, some, :, cut] = got.astype(BF16).reshape(4, bs, half)
                return carry
            lax.fori_loop(0, nsig // 4, fill_pot, 0)

    total_rows = nblk * rows
    step_rows = 2 * GROUP
    steps = total_rows // step_rows

    def fill_rhs(dest):
        for t in range(bpd):
            for batch in range(nb):
                rhs[t * bs:(t + 1) * bs, batch * npts:(batch + 1) * npts] = pot[
                    batch, inv_ref[batch, dest * bpd + t]
                ]

    def product(at):
        return lax.dot_general(
            lhs[pl.ds(at, step_rows), :], rhs[...], (((1,), (1,)), ((), ())), preferred_element_type=F32
        )

    def pair_copy(k):
        return remote(pair_send.at[k], pair_recv.at[k], pair_out.at[k], pair_in.at[k], (partner, z))

    def q_copy(k):
        return remote(q_send.at[k], q_recv.at[k], q_out.at[k], q_in.at[k], (peer(k), z))

    def s_copy(k):
        return remote(s_send.at[k], s_recv.at[k], s_out.at[k], s_in.at[k], (peer(k), z))

    for k in list(range(1, nchip)) + [0]:
        fill_rhs(lax.rem(chip + k, nchip) * CORES + (CORES - 1 - core))

        def theirs(i, carry):
            at = pl.multiple_of(i * step_rows, step_rows)
            pair_send[k, pl.ds(at, step_rows), :] = product(at)
            return carry
        lax.fori_loop(0, steps, theirs, 0)
        pair_copy(k).start()
        fill_rhs(lax.rem(chip + k, nchip) * CORES + core)
        pair_copy(k).wait_recv()

        def ours(i, carry):
            at = pl.multiple_of(i * step_rows, step_rows)
            value = product(at) + pair_recv[k, pl.ds(at, step_rows), :]
            if k == 0:
                out_ref[pl.ds(at, step_rows), :] = value
                return carry
            for g in range(2):
                some = value[g * GROUP:(g + 1) * GROUP]
                top = jnp.maximum(jnp.max(jnp.abs(some), axis=0, keepdims=True), TINY)
                s_send[k, i * 2 + g] = jnp.broadcast_to(top * (1.0 / LEVELS), (8, cols))
                q_send[k, pl.ds(pl.multiple_of(at + g * GROUP, GROUP), GROUP), :] = (
                    jnp.round(some * (LEVELS / top)).astype(jnp.int32).astype(jnp.int16)
                )
            return carry
        lax.fori_loop(0, steps, ours, 0)
        if k > 0:
            q_copy(k).start()
            s_copy(k).start()

    for k in range(1, nchip):
        q_copy(k).wait_recv()
        s_copy(k).wait_recv()

        def add(i, carry):
            at = pl.ds(pl.multiple_of(i * GROUP, GROUP), GROUP)
            out_ref[at, :] = out_ref[at, :] + q_recv[k, at, :].astype(jnp.int32).astype(F32) * s_recv[k, i, 0:1, :]
            return carry
        lax.fori_loop(0, total_rows // GROUP, add, 0)

    for k in range(nchip):
        p_forward(k).wait_send()
        pair_copy(k).wait_send()
        if k > 0:
            p_copy(k).wait_send()
            q_copy(k).wait_send()
            s_copy(k).wait_send()
    for owner in range(nrows):
        @pl.when(z != owner)
        def _():
            fm_copy(owner).wait_send()

        @pl.when(jnp.logical_and(z > 0, owner >= z))
        def _():
            for batch in range(nb):
                x_copy(batch, owner, -1).wait_send()
            m_copy(owner, -1).wait_send()

        @pl.when(jnp.logical_and(z < nrows - 1, owner <= z))
        def _():
            for batch in range(nb):
                x_copy(batch, owner, 1).wait_send()
            m_copy(owner, 1).wait_send()


def body(ngrid, nrows, density, basis_values, grid_points, grid_weights, screened_blocks):
    nblk, rows, cols = density.shape
    nb, nsig, _, npts = basis_values.shape
    bs = rows * nrows
    nchip = ngrid // CORES
    half = npts // (nrows // nb)
    total_rows = nblk * rows
    hit = screened_blocks[:, None, :] == jnp.arange(nblk, dtype=jnp.int32)[None, :, None]
    slot = jnp.arange(nsig, dtype=jnp.int32)
    inverse = jnp.min(jnp.where(hit, slot, nsig), axis=2).astype(jnp.int32)
    vmem = pl.BlockSpec(memory_space=pltpu.VMEM)
    smem = pl.BlockSpec(memory_space=pltpu.SMEM)
    dma = pltpu.SemaphoreType.DMA
    out = pl.pallas_call(
        functools.partial(kernel, ngrid, nrows),
        out_shape=jax.ShapeDtypeStruct((total_rows, cols), F32),
        in_specs=[smem] * 4 + [vmem] * 6,
        out_specs=vmem,
        scratch_shapes=[
            pltpu.VMEM((ngrid, nblk, cols // bs, rows, bs), BF16),
            pltpu.VMEM((nb, nsig, bs, npts), BF16),
            pltpu.VMEM((nsig * rows, nsig * bs), BF16),
            pltpu.VMEM((nrows, nsig, rows, half), BF16),
            pltpu.VMEM((nsig, bs, half), BF16),
            pltpu.VMEM((nrows, npts, half), BF16),
            pltpu.VMEM((nb, nsig + 1, rows, npts), BF16),
            pltpu.VMEM((nb, nsig + 1, bs, npts), BF16),
            pltpu.VMEM((total_rows, nb * npts), BF16),
            pltpu.VMEM((cols, nb * npts), BF16),
            pltpu.VMEM((nchip, total_rows, cols), F32),
            pltpu.VMEM((nchip, total_rows, cols), F32),
            pltpu.VMEM((nchip, total_rows, cols), jnp.int16),
            pltpu.VMEM((nchip, total_rows, cols), jnp.int16),
            pltpu.VMEM((nchip, total_rows // GROUP, 8, cols), F32),
            pltpu.VMEM((nchip, total_rows // GROUP, 8, cols), F32),
            dma((nchip,)), dma((nchip,)), dma((ngrid,)),
            dma((nb, nrows)), dma((nb, nrows)), dma((nb, nrows)),
            dma((1 + 2 * nb,)),
            dma((nrows,)), dma((nrows,)),
            dma((nrows,)), dma((nrows,)), dma((nrows,)),
            dma((nchip,)), dma((nchip,)), dma((nchip,)), dma((nchip,)), dma((nchip,)), dma((nchip,)),
        ],
        compiler_params=pltpu.CompilerParams(
            collective_id=0, has_side_effects=True, vmem_limit_bytes=63 * 1024 * 1024
        ),
        name="exchange",
    )(
        screened_blocks, screened_blocks // (cols // bs), screened_blocks % (cols // bs), inverse,
        density.reshape(nblk, rows, cols // bs, bs).swapaxes(1, 2), basis_values, grid_points, jnp.swapaxes(grid_points, 1, 2),
        grid_weights[:, None, :], grid_weights[:, :, None],
    )
    return out.reshape(nblk, rows, cols)


def solution(mesh):
    placed = (
        P(None, "rows", "grid"),
        P("grid", None, "rows", None),
        P("grid", None, None),
        P("grid", None),
        P("grid", None),
    )
    return jax.shard_map(
        functools.partial(body, mesh.shape["grid"], mesh.shape["rows"]), mesh=mesh, in_specs=placed,
        out_specs=P(None, "rows", "grid"), check_vma=False,
    )
```

```python
import functools

import jax
import jax.numpy as jnp
from jax import lax
from jax.experimental import pallas as pl
from jax.experimental.pallas import tpu as pltpu
from jax.sharding import PartitionSpec as P

MESH = pl.DeviceIdType.MESH
F32 = jnp.float32
BF16 = jnp.bfloat16
CORES = 2
GROUP = 128
LEVELS = 32767.0
TINY = 2.0 ** -110


def kernel(
    ngrid, nrows, sel_ref, inv_ref, p_ref, x_ref, pts_ref, w_ref, out_ref,
    p_mine, p_all, x_all, psel, fm_send, fm_all, mixed, xpad, pot, lhs, rhs, pair_send, pair_recv,
    q_send, q_recv, s_send, s_recv,
    p_out, p_pair, p_in, x_up, x_down, x_in, local, fm_out, fm_in, m_up, m_down, m_in,
    pair_out, pair_in, q_out, q_in, s_out, s_in,
):
    me = lax.axis_index("grid")
    z = lax.axis_index("rows")
    core = lax.rem(me, CORES)
    chip = me // CORES
    nchip = ngrid // CORES
    square = nchip == 4
    partner = chip * CORES + (CORES - 1 - core)
    nblk, rows, cols = p_ref.shape
    nb, nsig, _, npts = x_ref.shape
    bs = rows * nrows
    bpd = cols // bs
    split = nrows // nb
    half = npts // split
    pieces = 2
    part = nsig // pieces

    def toward(k):
        if square:
            return chip + (k % 2) * (1 - 2 * lax.rem(chip, 2)) + (k // 2) * (2 - 4 * (chip // 2))
        return lax.rem(chip + k, nchip)

    def source(k):
        return toward(k) if square else lax.rem(chip + nchip - k, nchip)

    def peer(k):
        return toward(k) * CORES + core

    def origin(k):
        return source(k) * CORES + core

    barrier = pltpu.get_barrier_semaphore()
    for k in range(1, nrows):
        pl.semaphore_signal(barrier, inc=1, device_id=(me, lax.rem(z + k, nrows)), device_id_type=MESH)
    for k in range(1, nchip):
        pl.semaphore_signal(barrier, inc=1, device_id=(peer(k), z), device_id_type=MESH)
    pl.semaphore_signal(barrier, inc=1, device_id=(partner, z), device_id_type=MESH)
    for t in range(bpd):
        p_mine[t] = p_ref[:, :, t * bs:(t + 1) * bs]
    pl.semaphore_wait(barrier, nrows - 1 + nchip - 1 + 1)

    def remote(src, dst, send, recv, device):
        return pltpu.make_async_remote_copy(
            src_ref=src, dst_ref=dst, send_sem=send, recv_sem=recv, device_id=device, device_id_type=MESH
        )

    def x_slot(batch, owner, c):
        return x_all.at[batch, pl.ds(c * part, part), pl.ds(pl.multiple_of(owner * rows, rows), rows), :]

    def x_copy(batch, owner, c, step, own=False):
        sems = x_up if step > 0 else x_down
        src = x_ref.at[batch, pl.ds(c * part, part)] if own else x_slot(batch, owner, c)
        return remote(
            src, x_slot(batch, owner, c), sems.at[batch, owner, c], x_in.at[batch, owner, c], (me, z + step)
        )

    def x_begin(batch):
        for c in range(pieces):
            @pl.when(z > 0)
            def _():
                x_copy(batch, z, c, -1, True).start()

            @pl.when(z < nrows - 1)
            def _():
                x_copy(batch, z, c, 1, True).start()

    def x_arrive(batch, dist):
        for c in range(pieces):
            @pl.when(z + dist < nrows)
            def _():
                x_copy(batch, z + dist, c, -1).wait_recv()

                @pl.when(z > 0)
                def _():
                    x_copy(batch, z + dist, c, -1).start()

            @pl.when(z - dist >= 0)
            def _():
                x_copy(batch, z - dist, c, 1).wait_recv()

                @pl.when(z < nrows - 1)
                def _():
                    x_copy(batch, z - dist, c, 1).start()

    def p_slot(owner):
        return p_all.at[pl.ds(owner * bpd, bpd)]

    def p_copy(k):
        return remote(p_mine, p_slot(me), p_out.at[k], p_in.at[me], (peer(k), z))

    def p_wait(k):
        return remote(p_mine, p_slot(origin(k)), p_out.at[k], p_in.at[origin(k)], (peer(k), z))

    def p_forward(k):
        src = p_mine if k == 0 else p_slot(origin(k))
        return remote(src, p_slot(origin(k)), p_pair.at[k], p_in.at[origin(k)], (partner, z))

    def p_pair_wait(k):
        slot = source(k) * CORES + (CORES - 1 - core)
        return remote(p_mine, p_slot(slot), p_pair.at[k], p_in.at[slot], (partner, z))

    x_begin(0)
    for k in range(1, nchip):
        p_copy(k).start()
    p_forward(0).start()

    locals_ = [pltpu.make_async_copy(p_mine, p_slot(me), local.at[0])]
    for batch in range(nb):
        for c in range(pieces):
            locals_.append(pltpu.make_async_copy(
                x_ref.at[batch, pl.ds(c * part, part)], x_slot(batch, z, c), local.at[1 + batch * pieces + c]
            ))
        locals_.append(pltpu.make_async_copy(
            x_ref.at[batch], xpad.at[batch, pl.ds(0, nsig)], local.at[1 + nb * pieces + batch]
        ))
    for copy in locals_:
        copy.start()
    for batch in range(nb):
        xpad[batch, nsig] = jnp.zeros((rows, npts), BF16)
        pot[batch, nsig] = jnp.zeros((bs, npts), BF16)
    for copy in locals_:
        copy.wait()

    for batch in range(nb):
        def fill(block, carry):
            lhs[pl.ds(pl.multiple_of(block * rows, rows), rows), batch * npts:(batch + 1) * npts] = xpad[
                batch, inv_ref[batch, block]
            ]
            return carry
        lax.fori_loop(0, nblk, fill, 0)

    def fm_slot(batch, owner):
        return fm_all.at[:, pl.ds(pl.multiple_of(owner * rows, rows), rows), :]

    def fm_copy(owner):
        return remote(fm_send.at[owner], fm_slot(0, z), fm_out.at[owner], fm_in.at[z], (me, owner))

    def fm_wait(other):
        return remote(fm_send.at[0], fm_slot(0, other), fm_out.at[0], fm_in.at[other], (me, other))

    def products(batch):
        def pick(s, carry):
            for t in range(nsig):
                psel[pl.ds(pl.multiple_of(s * rows, rows), rows), t * bs:(t + 1) * bs] = p_all[
                    sel_ref[batch, t], sel_ref[batch, s]
                ]
            return carry
        lax.fori_loop(0, nsig, pick, 0)
        for h in range(split):
            owner = batch * split + h
            got = jnp.dot(
                psel[...], x_all[batch, :, :, h * half:(h + 1) * half].reshape(nsig * bs, half),
                preferred_element_type=F32,
            )
            fm_send[owner] = got.astype(BF16).reshape(nsig, rows, half)
        for h in range(split):
            owner = batch * split + h

            @pl.when(z != owner)
            def _():
                fm_copy(owner).start()

            @pl.when(z == owner)
            def _():
                own = pltpu.make_async_copy(fm_send.at[owner], fm_slot(0, z), local.at[0])
                own.start()
                own.wait()

    def m_copy(owner, step):
        sems = m_up if step > 0 else m_down
        return remote(mixed.at[owner], mixed.at[owner], sems.at[owner], m_in.at[owner], (me, z + step))

    def mix(batch):
        @pl.when(z // split == batch)
        def _():
            for other in range(nrows):
                @pl.when(z != other)
                def _():
                    fm_wait(other).wait_recv()
            lanes = pl.ds(pl.multiple_of(lax.rem(z, split) * half, half), half)
            flipped = jnp.concatenate(
                [pts_ref[batch], w_ref[batch:batch + 1, :], jnp.zeros((4, npts), F32)], axis=0
            ).T
            tile = npts // 2
            for piece in range(2):
                q = slice(piece * tile, (piece + 1) * tile)
                inter = lax.dot_general(
                    x_all[batch, :, :, q].reshape(nsig * bs, tile), fm_all[...].reshape(nsig * bs, half),
                    (((0,), (0,)), ((), ())), preferred_element_type=F32,
                )
                dist2 = None
                for axis in range(3):
                    diff = flipped[q, axis:axis + 1] - pts_ref[batch, axis:axis + 1, lanes]
                    dist2 = diff * diff if dist2 is None else dist2 + diff * diff
                kern = 1.0 / jnp.sqrt(dist2 + 0.5)
                mixed[z, q, :] = (flipped[q, 3:4] * kern * inter).astype(BF16)

            @pl.when(z > 0)
            def _():
                m_copy(z, -1).start()

            @pl.when(z < nrows - 1)
            def _():
                m_copy(z, 1).start()

    def m_arrive(batch):
        for dist in range(1, nrows):
            from_up, from_down = z + dist, z - dist

            @pl.when(jnp.logical_and(from_up >= batch * split, from_up < (batch + 1) * split))
            def _():
                m_copy(from_up, -1).wait_recv()

                @pl.when(z > 0)
                def _():
                    m_copy(from_up, -1).start()

            @pl.when(jnp.logical_and(from_down >= batch * split, from_down < (batch + 1) * split))
            def _():
                m_copy(from_down, 1).wait_recv()

                @pl.when(z < nrows - 1)
                def _():
                    m_copy(from_down, 1).start()

    def potentials(batch):
        for h in range(split):
            cut = slice(h * half, (h + 1) * half)

            def fill_pot(i, carry):
                some = pl.ds(i * 4, 4)
                got = jnp.dot(
                    x_all[batch, some].reshape(4 * bs, npts), mixed[batch * split + h], preferred_element_type=F32
                ) * w_ref[batch:batch + 1, cut]
                pot[batch, some, :, cut] = got.astype(BF16).reshape(4, bs, half)
                return carry
            lax.fori_loop(0, nsig // 4, fill_pot, 0)

    for batch in range(nb):
        for dist in range(1, nrows - 1):
            x_arrive(batch, dist)
            if batch > 0 and dist == 1:
                products(batch - 1)
        if batch + 1 < nb:
            x_begin(batch + 1)
        if batch == 0:
            for k in range(1, nchip):
                p_wait(k).wait_recv()
                p_forward(k).start()
            for k in range(nchip):
                p_pair_wait(k).wait_recv()
        else:
            mix(batch - 1)
        x_arrive(batch, nrows - 1)
        if batch > 1:
            m_arrive(batch - 2)
    products(nb - 1)
    if nb > 1:
        m_arrive(nb - 2)
    mix(nb - 1)
    for batch in range(nb - 1):
        potentials(batch)
    m_arrive(nb - 1)
    potentials(nb - 1)

    total_rows = nblk * rows
    step_rows = min(4 * GROUP, total_rows)
    side = total_rows // 2

    def fill_rhs(dest):
        for t in range(bpd):
            for batch in range(nb):
                rhs[t * bs:(t + 1) * bs, batch * npts:(batch + 1) * npts] = pot[
                    batch, inv_ref[batch, dest * bpd + t]
                ]

    def product(at):
        return lax.dot_general(
            lhs[pl.ds(at, step_rows), :], rhs[...], (((1,), (1,)), ((), ())), preferred_element_type=F32
        )

    def pair_copy(k):
        return remote(pair_send.at[k], pair_recv.at[k], pair_out.at[k], pair_in.at[k], (partner, z))

    def q_copy(k, cut, device):
        at = pl.ds(cut * side, side)
        return remote(q_send.at[k, at], q_recv.at[k, at], q_out.at[k, cut], q_in.at[k, cut], (device, z))

    def s_copy(k, cut, device):
        at = pl.ds(cut * (side // GROUP), side // GROUP)
        return remote(s_send.at[k, at], s_recv.at[k, at], s_out.at[k, cut], s_in.at[k, cut], (device, z))

    def send(k, cut, device):
        q_copy(k, cut, device).start()
        s_copy(k, cut, device).start()

    def arrive(k, cut, device):
        q_copy(k, cut, device).wait_recv()
        s_copy(k, cut, device).wait_recv()

    def encode(k, group, some):
        top = jnp.maximum(jnp.max(jnp.abs(some), axis=0, keepdims=True), TINY)
        s_send[k, group] = jnp.broadcast_to(top * (1.0 / LEVELS), (8, cols))
        q_send[k, pl.ds(pl.multiple_of(group * GROUP, GROUP), GROUP), :] = (
            jnp.round(some * (LEVELS / top)).astype(jnp.int32).astype(jnp.int16)
        )

    def decode(k, group):
        at = pl.ds(pl.multiple_of(group * GROUP, GROUP), GROUP)
        return q_recv[k, at, :].astype(jnp.int32).astype(F32) * s_recv[k, group, 0:1, :]

    def start_pair(k):
        fill_rhs(toward(k) * CORES + (CORES - 1 - core))

        def theirs(i, carry):
            at = pl.multiple_of(i * step_rows, step_rows)
            pair_send[k, pl.ds(at, step_rows), :] = product(at)
            return carry
        lax.fori_loop(0, total_rows // step_rows, theirs, 0)
        pair_copy(k).start()

    def finish_pair(k, keep):
        fill_rhs(toward(k) * CORES + core)
        pair_copy(k).wait_recv()

        def ours(i, carry):
            at = pl.multiple_of(i * step_rows, step_rows)
            value = product(at) + pair_recv[k, pl.ds(at, step_rows), :]
            keep(k, i, at, value)
            return carry
        lax.fori_loop(0, total_rows // step_rows, ours, 0)

    def keep_code(k, i, at, value):
        for g in range(step_rows // GROUP):
            encode(k, i * (step_rows // GROUP) + g, value[g * GROUP:(g + 1) * GROUP])

    def keep_value(k, i, at, value):
        pair_recv[k, pl.ds(at, step_rows), :] = value

    def keep_out(k, i, at, value):
        out_ref[pl.ds(at, step_rows), :] = value

    def groups(cut, step):
        def one(i, carry):
            step(cut * (side // GROUP) + i)
            return carry
        lax.fori_loop(0, side // GROUP, one, 0)

    def add(k, cut):
        def one(group):
            at = pl.ds(pl.multiple_of(group * GROUP, GROUP), GROUP)
            out_ref[at, :] = out_ref[at, :] + decode(k, group)
        groups(cut, one)

    def rows_of(k, group):
        return pair_recv[k, pl.ds(pl.multiple_of(group * GROUP, GROUP), GROUP), :]

    if square:
        flip = {1: peer(1), 2: peer(2)}
        start_pair(3)
        finish_pair(3, keep_code)
        for cut in range(2):
            send(3, cut, flip[cut + 1])
        for k in (1, 2):
            start_pair(k)
            finish_pair(k, keep_value)
            groups(k - 1, lambda group: encode(k, group, rows_of(k, group)))
            send(k, k - 1, flip[k])
        start_pair(0)
        finish_pair(0, keep_out)
        for k in (1, 2):
            cut = 2 - k
            arrive(3, cut, flip[3 - k])
            groups(cut, lambda group: encode(k, group, rows_of(k, group) + decode(3, group)))
            send(k, cut, flip[k])
        for k in (1, 2):
            arrive(k, k - 1, flip[k])
            add(k, k - 1)
        for k in (1, 2):
            arrive(k, 2 - k, flip[k])
            add(k, 2 - k)
        sent = [(3, 0, flip[1]), (3, 1, flip[2])] + [(k, cut, flip[k]) for k in (1, 2) for cut in range(2)]
    else:
        for k in list(range(1, nchip)):
            start_pair(k)
            finish_pair(k, keep_code)
            for cut in range(2):
                send(k, cut, peer(k))
        start_pair(0)
        finish_pair(0, keep_out)
        for k in range(1, nchip):
            for cut in range(2):
                arrive(k, cut, peer(k))
                add(k, cut)
        sent = [(k, cut, peer(k)) for k in range(1, nchip) for cut in range(2)]

    for k, cut, device in sent:
        q_copy(k, cut, device).wait_send()
        s_copy(k, cut, device).wait_send()
    for k in range(nchip):
        p_forward(k).wait_send()
        pair_copy(k).wait_send()
        if k > 0:
            p_copy(k).wait_send()
    for owner in range(nrows):
        @pl.when(z != owner)
        def _():
            fm_copy(owner).wait_send()

        @pl.when(jnp.logical_and(z > 0, owner >= z))
        def _():
            for batch in range(nb):
                for c in range(pieces):
                    x_copy(batch, owner, c, -1).wait_send()
            m_copy(owner, -1).wait_send()

        @pl.when(jnp.logical_and(z < nrows - 1, owner <= z))
        def _():
            for batch in range(nb):
                for c in range(pieces):
                    x_copy(batch, owner, c, 1).wait_send()
            m_copy(owner, 1).wait_send()


def body(ngrid, nrows, density, basis_values, grid_points, grid_weights, screened_blocks):
    nblk, rows, cols = density.shape
    nb, nsig, _, npts = basis_values.shape
    bs = rows * nrows
    nchip = ngrid // CORES
    half = npts // (nrows // nb)
    total_rows = nblk * rows
    hit = screened_blocks[:, None, :] == jnp.arange(nblk, dtype=jnp.int32)[None, :, None]
    slot = jnp.arange(nsig, dtype=jnp.int32)
    inverse = jnp.min(jnp.where(hit, slot, nsig), axis=2).astype(jnp.int32)
    vmem = pl.BlockSpec(memory_space=pltpu.VMEM)
    smem = pl.BlockSpec(memory_space=pltpu.SMEM)
    dma = pltpu.SemaphoreType.DMA
    out = pl.pallas_call(
        functools.partial(kernel, ngrid, nrows),
        out_shape=jax.ShapeDtypeStruct((total_rows, cols), F32),
        in_specs=[smem, smem] + [vmem] * 4,
        out_specs=vmem,
        scratch_shapes=[
            pltpu.VMEM((cols // bs, nblk, rows, bs), BF16),
            pltpu.VMEM((nblk, nblk, rows, bs), BF16),
            pltpu.VMEM((nb, nsig, bs, npts), BF16),
            pltpu.VMEM((nsig * rows, nsig * bs), BF16),
            pltpu.VMEM((nrows, nsig, rows, half), BF16),
            pltpu.VMEM((nsig, bs, half), BF16),
            pltpu.VMEM((nrows, npts, half), BF16),
            pltpu.VMEM((nb, nsig + 1, rows, npts), BF16),
            pltpu.VMEM((nb, nsig + 1, bs, npts), BF16),
            pltpu.VMEM((total_rows, nb * npts), BF16),
            pltpu.VMEM((cols, nb * npts), BF16),
            pltpu.VMEM((nchip, total_rows, cols), F32),
            pltpu.VMEM((nchip, total_rows, cols), F32),
            pltpu.VMEM((nchip, total_rows, cols), jnp.int16),
            pltpu.VMEM((nchip, total_rows, cols), jnp.int16),
            pltpu.VMEM((nchip, total_rows // GROUP, 8, cols), F32),
            pltpu.VMEM((nchip, total_rows // GROUP, 8, cols), F32),
            dma((nchip,)), dma((nchip,)), dma((ngrid,)),
            dma((nb, nrows, 2)), dma((nb, nrows, 2)), dma((nb, nrows, 2)),
            dma((1 + 3 * nb,)),
            dma((nrows,)), dma((nrows,)),
            dma((nrows,)), dma((nrows,)), dma((nrows,)),
            dma((nchip,)), dma((nchip,)),
            dma((nchip, 2)), dma((nchip, 2)), dma((nchip, 2)), dma((nchip, 2)),
        ],
        compiler_params=pltpu.CompilerParams(
            collective_id=0, has_side_effects=True, vmem_limit_bytes=63 * 1024 * 1024
        ),
        name="exchange",
    )(screened_blocks, inverse, density, basis_values, grid_points, grid_weights)
    return out.reshape(nblk, rows, cols)


def solution(mesh):
    placed = (
        P(None, "rows", "grid"),
        P("grid", None, "rows", None),
        P("grid", None, None),
        P("grid", None),
        P("grid", None),
    )
    return jax.shard_map(
        functools.partial(body, mesh.shape["grid"], mesh.shape["rows"]), mesh=mesh, in_specs=placed,
        out_specs=P(None, "rows", "grid"), check_vma=False,
    )
```

```python
import functools

import jax
import jax.numpy as jnp
from jax import lax
from jax.experimental import pallas as pl
from jax.experimental.pallas import tpu as pltpu
from jax.sharding import PartitionSpec as P

MESH = pl.DeviceIdType.MESH
F32 = jnp.float32
BF16 = jnp.bfloat16
CORES = 2
GROUP = 128
LEVELS = 32767.0
TINY = 2.0 ** -110


def kernel(
    ngrid, nrows, sel_ref, inv_ref, p_ref, x_ref, pts_ref, w_ref, out_ref,
    p_mine, p_all, x_all, psel, fm_send, fm_all, mixed, xpad, pot, lhs, rhs, pair_send, pair_recv,
    q_send, q_recv, s_send, s_recv,
    p_out, p_pair, p_in, x_up, x_down, x_in, local, fm_out, fm_in, m_up, m_down, m_in,
    pair_out, pair_in, q_out, q_in, s_out, s_in,
):
    me = lax.axis_index("grid")
    z = lax.axis_index("rows")
    core = lax.rem(me, CORES)
    chip = me // CORES
    nchip = ngrid // CORES
    square = nchip == 4
    partner = chip * CORES + (CORES - 1 - core)
    nblk, rows, cols = p_ref.shape
    nb, nsig, _, npts = x_ref.shape
    bs = rows * nrows
    bpd = cols // bs
    split = nrows // nb
    half = npts // split
    pieces = 1
    part = nsig // pieces

    def toward(k):
        if square:
            return chip + (k % 2) * (1 - 2 * lax.rem(chip, 2)) + (k // 2) * (2 - 4 * (chip // 2))
        return lax.rem(chip + k, nchip)

    def source(k):
        return toward(k) if square else lax.rem(chip + nchip - k, nchip)

    def peer(k):
        return toward(k) * CORES + core

    def origin(k):
        return source(k) * CORES + core

    barrier = pltpu.get_barrier_semaphore()
    for k in range(1, nrows):
        pl.semaphore_signal(barrier, inc=1, device_id=(me, lax.rem(z + k, nrows)), device_id_type=MESH)
    for k in range(1, nchip):
        pl.semaphore_signal(barrier, inc=1, device_id=(peer(k), z), device_id_type=MESH)
    pl.semaphore_signal(barrier, inc=1, device_id=(partner, z), device_id_type=MESH)
    for t in range(bpd):
        p_mine[t] = p_ref[:, :, t * bs:(t + 1) * bs]
    pl.semaphore_wait(barrier, nrows - 1 + nchip - 1 + 1)

    def remote(src, dst, send, recv, device):
        return pltpu.make_async_remote_copy(
            src_ref=src, dst_ref=dst, send_sem=send, recv_sem=recv, device_id=device, device_id_type=MESH
        )

    def x_slot(batch, owner, c):
        return x_all.at[batch, pl.ds(c * part, part), pl.ds(pl.multiple_of(owner * rows, rows), rows), :]

    def x_copy(batch, owner, c, step, own=False):
        sems = x_up if step > 0 else x_down
        src = x_ref.at[batch, pl.ds(c * part, part)] if own else x_slot(batch, owner, c)
        return remote(
            src, x_slot(batch, owner, c), sems.at[batch, owner, c], x_in.at[batch, owner, c], (me, z + step)
        )

    def x_begin(batch):
        for c in range(pieces):
            @pl.when(z > 0)
            def _():
                x_copy(batch, z, c, -1, True).start()

            @pl.when(z < nrows - 1)
            def _():
                x_copy(batch, z, c, 1, True).start()

    def x_arrive(batch, dist):
        for c in range(pieces):
            @pl.when(z + dist < nrows)
            def _():
                x_copy(batch, z + dist, c, -1).wait_recv()

                @pl.when(z > 0)
                def _():
                    x_copy(batch, z + dist, c, -1).start()

            @pl.when(z - dist >= 0)
            def _():
                x_copy(batch, z - dist, c, 1).wait_recv()

                @pl.when(z < nrows - 1)
                def _():
                    x_copy(batch, z - dist, c, 1).start()

    def p_slot(owner):
        return p_all.at[pl.ds(owner * bpd, bpd)]

    def p_copy(k):
        return remote(p_mine, p_slot(me), p_out.at[k], p_in.at[me], (peer(k), z))

    def p_wait(k):
        return remote(p_mine, p_slot(origin(k)), p_out.at[k], p_in.at[origin(k)], (peer(k), z))

    def p_forward(k):
        src = p_mine if k == 0 else p_slot(origin(k))
        return remote(src, p_slot(origin(k)), p_pair.at[k], p_in.at[origin(k)], (partner, z))

    def p_pair_wait(k):
        slot = source(k) * CORES + (CORES - 1 - core)
        return remote(p_mine, p_slot(slot), p_pair.at[k], p_in.at[slot], (partner, z))

    for batch in range(nb):
        x_begin(batch)
    for k in range(1, nchip):
        p_copy(k).start()
    p_forward(0).start()

    locals_ = [pltpu.make_async_copy(p_mine, p_slot(me), local.at[0])]
    for batch in range(nb):
        for c in range(pieces):
            locals_.append(pltpu.make_async_copy(
                x_ref.at[batch, pl.ds(c * part, part)], x_slot(batch, z, c), local.at[1 + batch * pieces + c]
            ))
        locals_.append(pltpu.make_async_copy(
            x_ref.at[batch], xpad.at[batch, pl.ds(0, nsig)], local.at[1 + nb * pieces + batch]
        ))
    for copy in locals_:
        copy.start()
    for batch in range(nb):
        xpad[batch, nsig] = jnp.zeros((rows, npts), BF16)
        pot[batch, nsig] = jnp.zeros((bs, npts), BF16)
    for copy in locals_:
        copy.wait()

    for batch in range(nb):
        def fill(block, carry):
            lhs[pl.ds(pl.multiple_of(block * rows, rows), rows), batch * npts:(batch + 1) * npts] = xpad[
                batch, inv_ref[batch, block]
            ]
            return carry
        lax.fori_loop(0, nblk, fill, 0)

    def fm_slot(batch, owner):
        return fm_all.at[:, pl.ds(pl.multiple_of(owner * rows, rows), rows), :]

    def fm_copy(owner):
        return remote(fm_send.at[owner], fm_slot(0, z), fm_out.at[owner], fm_in.at[z], (me, owner))

    def fm_wait(other):
        return remote(fm_send.at[0], fm_slot(0, other), fm_out.at[0], fm_in.at[other], (me, other))

    def products(batch):
        def pick(s, carry):
            for t in range(nsig):
                psel[pl.ds(pl.multiple_of(s * rows, rows), rows), t * bs:(t + 1) * bs] = p_all[
                    sel_ref[batch, t], sel_ref[batch, s]
                ]
            return carry
        lax.fori_loop(0, nsig, pick, 0)
        for h in range(split):
            owner = batch * split + h
            got = jnp.dot(
                psel[...], x_all[batch, :, :, h * half:(h + 1) * half].reshape(nsig * bs, half),
                preferred_element_type=F32,
            )
            fm_send[owner] = got.astype(BF16).reshape(nsig, rows, half)
        for h in range(split):
            owner = batch * split + h

            @pl.when(z != owner)
            def _():
                fm_copy(owner).start()

            @pl.when(z == owner)
            def _():
                own = pltpu.make_async_copy(fm_send.at[owner], fm_slot(0, z), local.at[0])
                own.start()
                own.wait()

    def m_copy(owner, step):
        sems = m_up if step > 0 else m_down
        return remote(mixed.at[owner], mixed.at[owner], sems.at[owner], m_in.at[owner], (me, z + step))

    def mix(batch):
        @pl.when(z // split == batch)
        def _():
            for other in range(nrows):
                @pl.when(z != other)
                def _():
                    fm_wait(other).wait_recv()
            lanes = pl.ds(pl.multiple_of(lax.rem(z, split) * half, half), half)
            flipped = jnp.concatenate(
                [pts_ref[batch], w_ref[batch:batch + 1, :], jnp.zeros((4, npts), F32)], axis=0
            ).T
            tile = npts // 2
            for piece in range(2):
                q = slice(piece * tile, (piece + 1) * tile)
                inter = lax.dot_general(
                    x_all[batch, :, :, q].reshape(nsig * bs, tile), fm_all[...].reshape(nsig * bs, half),
                    (((0,), (0,)), ((), ())), preferred_element_type=F32,
                )
                dist2 = None
                for axis in range(3):
                    diff = flipped[q, axis:axis + 1] - pts_ref[batch, axis:axis + 1, lanes]
                    dist2 = diff * diff if dist2 is None else dist2 + diff * diff
                kern = 1.0 / jnp.sqrt(dist2 + 0.5)
                mixed[z, q, :] = (flipped[q, 3:4] * kern * inter).astype(BF16)

            @pl.when(z > 0)
            def _():
                m_copy(z, -1).start()

            @pl.when(z < nrows - 1)
            def _():
                m_copy(z, 1).start()

    def m_arrive():
        for dist in range(1, nrows):
            from_up, from_down = z + dist, z - dist

            @pl.when(from_up < nrows)
            def _():
                m_copy(from_up, -1).wait_recv()

                @pl.when(z > 0)
                def _():
                    m_copy(from_up, -1).start()

            @pl.when(from_down >= 0)
            def _():
                m_copy(from_down, 1).wait_recv()

                @pl.when(z < nrows - 1)
                def _():
                    m_copy(from_down, 1).start()

    def potentials(batch):
        for h in range(split):
            cut = slice(h * half, (h + 1) * half)

            def fill_pot(i, carry):
                some = pl.ds(i * 4, 4)
                got = jnp.dot(
                    x_all[batch, some].reshape(4 * bs, npts), mixed[batch * split + h], preferred_element_type=F32
                ) * w_ref[batch:batch + 1, cut]
                pot[batch, some, :, cut] = got.astype(BF16).reshape(4, bs, half)
                return carry
            lax.fori_loop(0, nsig // 4, fill_pot, 0)

    for dist in range(1, nrows - 1):
        for batch in range(nb):
            x_arrive(batch, dist)
    for k in range(1, nchip):
        p_wait(k).wait_recv()
        p_forward(k).start()
    for k in range(nchip):
        p_pair_wait(k).wait_recv()
    for batch in range(nb):
        x_arrive(batch, nrows - 1)
        products(batch)
    for batch in range(nb):
        mix(batch)
    m_arrive()
    for batch in range(nb):
        potentials(batch)

    total_rows = nblk * rows
    step_rows = min(4 * GROUP, total_rows)
    side = total_rows // 2

    def fill_rhs(dest):
        for t in range(bpd):
            for batch in range(nb):
                rhs[t * bs:(t + 1) * bs, batch * npts:(batch + 1) * npts] = pot[
                    batch, inv_ref[batch, dest * bpd + t]
                ]

    def product(at):
        return lax.dot_general(
            lhs[pl.ds(at, step_rows), :], rhs[...], (((1,), (1,)), ((), ())), preferred_element_type=F32
        )

    def pair_copy(k):
        return remote(pair_send.at[k], pair_recv.at[k], pair_out.at[k], pair_in.at[k], (partner, z))

    def q_copy(k, cut, device):
        at = pl.ds(cut * side, side)
        return remote(q_send.at[k, at], q_recv.at[k, at], q_out.at[k, cut], q_in.at[k, cut], (device, z))

    def s_copy(k, cut, device):
        at = pl.ds(cut * (side // GROUP), side // GROUP)
        return remote(s_send.at[k, at], s_recv.at[k, at], s_out.at[k, cut], s_in.at[k, cut], (device, z))

    def send(k, cut, device):
        q_copy(k, cut, device).start()
        s_copy(k, cut, device).start()

    def arrive(k, cut, device):
        q_copy(k, cut, device).wait_recv()
        s_copy(k, cut, device).wait_recv()

    def encode(k, group, some):
        top = jnp.maximum(jnp.max(jnp.abs(some), axis=0, keepdims=True), TINY)
        s_send[k, group] = jnp.broadcast_to(top * (1.0 / LEVELS), (8, cols))
        q_send[k, pl.ds(pl.multiple_of(group * GROUP, GROUP), GROUP), :] = (
            jnp.round(some * (LEVELS / top)).astype(jnp.int32).astype(jnp.int16)
        )

    def decode(k, group):
        at = pl.ds(pl.multiple_of(group * GROUP, GROUP), GROUP)
        return q_recv[k, at, :].astype(jnp.int32).astype(F32) * s_recv[k, group, 0:1, :]

    def start_pair(k):
        fill_rhs(toward(k) * CORES + (CORES - 1 - core))

        def theirs(i, carry):
            at = pl.multiple_of(i * step_rows, step_rows)
            pair_send[k, pl.ds(at, step_rows), :] = product(at)
            return carry
        lax.fori_loop(0, total_rows // step_rows, theirs, 0)
        pair_copy(k).start()

    def finish_pair(k, keep):
        fill_rhs(toward(k) * CORES + core)
        pair_copy(k).wait_recv()

        def ours(i, carry):
            at = pl.multiple_of(i * step_rows, step_rows)
            value = product(at) + pair_recv[k, pl.ds(at, step_rows), :]
            keep(k, i, at, value)
            return carry
        lax.fori_loop(0, total_rows // step_rows, ours, 0)

    def keep_code(k, i, at, value):
        for g in range(step_rows // GROUP):
            encode(k, i * (step_rows // GROUP) + g, value[g * GROUP:(g + 1) * GROUP])

    def keep_value(k, i, at, value):
        pair_recv[k, pl.ds(at, step_rows), :] = value

    def keep_out(k, i, at, value):
        out_ref[pl.ds(at, step_rows), :] = value

    def groups(cut, step):
        def one(i, carry):
            step(cut * (side // GROUP) + i)
            return carry
        lax.fori_loop(0, side // GROUP, one, 0)

    def add(k, cut):
        def one(group):
            at = pl.ds(pl.multiple_of(group * GROUP, GROUP), GROUP)
            out_ref[at, :] = out_ref[at, :] + decode(k, group)
        groups(cut, one)

    def rows_of(k, group):
        return pair_recv[k, pl.ds(pl.multiple_of(group * GROUP, GROUP), GROUP), :]

    if square:
        flip = {1: peer(1), 2: peer(2)}
        start_pair(3)
        finish_pair(3, keep_code)
        for cut in range(2):
            send(3, cut, flip[cut + 1])
        for k in (1, 2):
            start_pair(k)
            finish_pair(k, keep_value)
            groups(k - 1, lambda group: encode(k, group, rows_of(k, group)))
            send(k, k - 1, flip[k])
        start_pair(0)
        finish_pair(0, keep_out)
        for k in (1, 2):
            cut = 2 - k
            arrive(3, cut, flip[3 - k])
            groups(cut, lambda group: encode(k, group, rows_of(k, group) + decode(3, group)))
            send(k, cut, flip[k])
        for k in (1, 2):
            arrive(k, k - 1, flip[k])
            add(k, k - 1)
        for k in (1, 2):
            arrive(k, 2 - k, flip[k])
            add(k, 2 - k)
        sent = [(3, 0, flip[1]), (3, 1, flip[2])] + [(k, cut, flip[k]) for k in (1, 2) for cut in range(2)]
    else:
        for k in list(range(1, nchip)):
            start_pair(k)
            finish_pair(k, keep_code)
            for cut in range(2):
                send(k, cut, peer(k))
        start_pair(0)
        finish_pair(0, keep_out)
        for k in range(1, nchip):
            for cut in range(2):
                arrive(k, cut, peer(k))
                add(k, cut)
        sent = [(k, cut, peer(k)) for k in range(1, nchip) for cut in range(2)]

    for k, cut, device in sent:
        q_copy(k, cut, device).wait_send()
        s_copy(k, cut, device).wait_send()
    for k in range(nchip):
        p_forward(k).wait_send()
        pair_copy(k).wait_send()
        if k > 0:
            p_copy(k).wait_send()
    for owner in range(nrows):
        @pl.when(z != owner)
        def _():
            fm_copy(owner).wait_send()

        @pl.when(jnp.logical_and(z > 0, owner >= z))
        def _():
            for batch in range(nb):
                for c in range(pieces):
                    x_copy(batch, owner, c, -1).wait_send()
            m_copy(owner, -1).wait_send()

        @pl.when(jnp.logical_and(z < nrows - 1, owner <= z))
        def _():
            for batch in range(nb):
                for c in range(pieces):
                    x_copy(batch, owner, c, 1).wait_send()
            m_copy(owner, 1).wait_send()


def body(ngrid, nrows, density, basis_values, grid_points, grid_weights, screened_blocks):
    nblk, rows, cols = density.shape
    nb, nsig, _, npts = basis_values.shape
    bs = rows * nrows
    nchip = ngrid // CORES
    half = npts // (nrows // nb)
    total_rows = nblk * rows
    hit = screened_blocks[:, None, :] == jnp.arange(nblk, dtype=jnp.int32)[None, :, None]
    slot = jnp.arange(nsig, dtype=jnp.int32)
    inverse = jnp.min(jnp.where(hit, slot, nsig), axis=2).astype(jnp.int32)
    vmem = pl.BlockSpec(memory_space=pltpu.VMEM)
    smem = pl.BlockSpec(memory_space=pltpu.SMEM)
    dma = pltpu.SemaphoreType.DMA
    out = pl.pallas_call(
        functools.partial(kernel, ngrid, nrows),
        out_shape=jax.ShapeDtypeStruct((total_rows, cols), F32),
        in_specs=[smem, smem] + [vmem] * 4,
        out_specs=vmem,
        scratch_shapes=[
            pltpu.VMEM((cols // bs, nblk, rows, bs), BF16),
            pltpu.VMEM((nblk, nblk, rows, bs), BF16),
            pltpu.VMEM((nb, nsig, bs, npts), BF16),
            pltpu.VMEM((nsig * rows, nsig * bs), BF16),
            pltpu.VMEM((nrows, nsig, rows, half), BF16),
            pltpu.VMEM((nsig, bs, half), BF16),
            pltpu.VMEM((nrows, npts, half), BF16),
            pltpu.VMEM((nb, nsig + 1, rows, npts), BF16),
            pltpu.VMEM((nb, nsig + 1, bs, npts), BF16),
            pltpu.VMEM((total_rows, nb * npts), BF16),
            pltpu.VMEM((cols, nb * npts), BF16),
            pltpu.VMEM((nchip, total_rows, cols), F32),
            pltpu.VMEM((nchip, total_rows, cols), F32),
            pltpu.VMEM((nchip, total_rows, cols), jnp.int16),
            pltpu.VMEM((nchip, total_rows, cols), jnp.int16),
            pltpu.VMEM((nchip, total_rows // GROUP, 8, cols), F32),
            pltpu.VMEM((nchip, total_rows // GROUP, 8, cols), F32),
            dma((nchip,)), dma((nchip,)), dma((ngrid,)),
            dma((nb, nrows, 2)), dma((nb, nrows, 2)), dma((nb, nrows, 2)),
            dma((1 + 3 * nb,)),
            dma((nrows,)), dma((nrows,)),
            dma((nrows,)), dma((nrows,)), dma((nrows,)),
            dma((nchip,)), dma((nchip,)),
            dma((nchip, 2)), dma((nchip, 2)), dma((nchip, 2)), dma((nchip, 2)),
        ],
        compiler_params=pltpu.CompilerParams(
            collective_id=0, has_side_effects=True, vmem_limit_bytes=63 * 1024 * 1024
        ),
        name="exchange",
    )(screened_blocks, inverse, density, basis_values, grid_points, grid_weights)
    return out.reshape(nblk, rows, cols)


def solution(mesh):
    placed = (
        P(None, "rows", "grid"),
        P("grid", None, "rows", None),
        P("grid", None, None),
        P("grid", None),
        P("grid", None),
    )
    return jax.shard_map(
        functools.partial(body, mesh.shape["grid"], mesh.shape["rows"]), mesh=mesh, in_specs=placed,
        out_specs=P(None, "rows", "grid"), check_vma=False,
    )
```
